32 devices in a mesh: row: 8 (over y, x, core), col: 4 (over z).
Axes of the slice: x: 2, y: 2, z: 4, core: 2. Of those that a mesh axis runs over, the one named last changes fastest.
Arguments:
- history: float32 [3, 512, 4096], P(None, None, ('row', 'col')), may hold values from -8 to 8
Outputs:
- orbitals: float32 [512, 4096], P(None, ('row', 'col'))
The draws below stay inside these ranges and needn't reach their ends.
All inputs are finite; a program needn't handle non-finite values.
Results may differ from the reference program's by a relative error of at most 0.0003.
Values sent between devices are 32-bit elements; how exact they have to be, the bound alone decides.
A program may use at most 64 MiB of HBM per device.

```python
import jax
import jax.numpy as jnp
from jax import lax

NORB = 512
NHIST = 3
NPW = 4096


def draw_history(key, part):
    base_key = jax.random.fold_in(key, 11)
    base = jax.random.truncated_normal(base_key, -4.0, 4.0, (NORB, NPW), jnp.float32)
    drifts = jax.random.truncated_normal(jax.random.fold_in(key, 13), -4.0, 4.0, (NHIST, NORB, NPW), jnp.float32)
    return base[None, :, :] + 0.35 * drifts


def setup_inputs(seed: int = 0) -> dict:
    splits = jax.random.split(jax.random.key(seed), 2)
    history = draw_history(jax.random.fold_in(splits[1], 71), 0)
    return {"history": history}


def reference(history):
    precise = lax.Precision.HIGHEST
    npw_total = history.shape[2]
    newest = history[0]
    weights = (2.5, -2.0, 0.5)
    predicted = jnp.zeros(newest.shape, jnp.float32)
    for index in range(3):
        project = jnp.einsum('ip,jp->ij', newest, history[index], precision=precise) / npw_total
        predicted = predicted + weights[index] * jnp.dot(project, history[index], precision=precise)
    gram = jnp.einsum('ip,jp->ij', predicted, predicted, precision=precise) / npw_total
    factor = jnp.linalg.cholesky(gram)
    return lax.linalg.triangular_solve(factor, predicted, left_side=True, lower=True)
```

```python
import functools

import jax
import jax.numpy as jnp
import numpy as np
from jax import lax
from jax.experimental import pallas as pl
from jax.experimental.pallas import tpu as pltpu
from jax.sharding import PartitionSpec as P

MESH = pl.DeviceIdType.MESH
B = 128
STREAMS = 3
WEIGHTS = (2.5, -2.0, 0.5)
NT = (((1,), (1,)), ((), ()))
NN = (((1,), (0,)), ((), ()))


def split(x):
    high = x.astype(jnp.bfloat16)
    return high, (x - high.astype(jnp.float32)).astype(jnp.bfloat16)


def dot3(a, b, dims):
    mul = functools.partial(lax.dot_general, dimension_numbers=dims, preferred_element_type=jnp.float32)
    return mul(a[0], b[0]) + (mul(a[0], b[1]) + mul(a[1], b[0]))


def exchange_orders(n_row, n_col):
    row = [("row", bit) for bit in range(1, n_row.bit_length() - 1)]
    col = [("col", bit) for bit in range(n_col.bit_length() - 1)]
    half = (len(row) + 1) // 2
    parts = [row[:half], row[half:], col]
    first = [("row", 0)]
    return [first + parts[s] + parts[(s + 1) % 3] + parts[(s + 2) % 3] for s in range(STREAMS)]


def plan(rows, stages, halvings):
    steps, offset = [], 0
    for stage in range(stages):
        halve = stage < halvings and rows % 16 == 0 and rows >= 16
        if halve:
            rows //= 2
        steps.append((halve, rows, offset))
        offset += rows
    return steps, offset


def layout(blocks):
    place, counts = {}, []
    for stream, part in enumerate(np.array_split(np.arange(len(blocks)), STREAMS)):
        counts.append(len(part))
        for slot, index in enumerate(part):
            place[blocks[index]] = (stream, slot * B)
    return place, counts


def projection_blocks(nb):
    return [(0, i, k) for i in range(nb) for k in range(i + 1)] + [
        (j, i, k) for j in (1, 2) for i in range(nb) for k in range(nb)
    ]


def gram_blocks(nb):
    return [(i, k) for i in range(nb) for k in range(i + 1)]


class Reducer:
    def __init__(self, accs, recvs, sums, send_sem, recv_sem, gsend_sem, grecv_sem, orders, plans):
        self.accs, self.recvs, self.sums, self.orders, self.plans = accs, recvs, sums, orders, plans
        self.sems = (send_sem, recv_sem, gsend_sem, grecv_sem)
        self.off = [0] * len(accs)
        self.parent = [[] for _ in accs]
        self.copies = {}
        self.index = {axis: lax.axis_index(axis) for axis in ("row", "col")}

    def partner(self, axis, bit):
        me = self.index[axis]
        side = lax.rem(lax.div(me, 1 << bit), 2)
        other = me + (1 - 2 * side) * (1 << bit)
        device = (other, self.index["col"]) if axis == "row" else (self.index["row"], other)
        return side, device

    def start(self, s, t):
        side, device = self.partner(*self.orders[s][t])
        halve, rows, at = self.plans[s][t]
        off = self.off[s]
        self.parent[s].append(off)
        sent = off
        if halve:
            sent = pl.multiple_of(off + (1 - side) * rows, 8)
            self.off[s] = pl.multiple_of(off + side * rows, 8)
        copy = pltpu.make_async_remote_copy(
            src_ref=self.accs[s].at[pl.ds(sent, rows)],
            dst_ref=self.recvs[s].at[pl.ds(at, rows)],
            send_sem=self.sems[0].at[s, t],
            recv_sem=self.sems[1].at[s, t],
            device_id=device,
            device_id_type=MESH,
        )
        copy.start()
        self.copies[s] = copy

    def finish(self, s, t):
        self.copies[s].wait()
        _, rows, at = self.plans[s][t]
        here = pl.ds(self.off[s], rows)
        target = self.sums[s] if t + 1 == len(self.orders[s]) else self.accs[s]
        target[here] = self.accs[s][here] + self.recvs[s][pl.ds(at, rows)]

    def run(self):
        stages = len(self.orders[0])
        streams = range(len(self.accs))
        for t in range(stages):
            for s in streams:
                self.finish(s, t)
                if t + 1 < stages:
                    self.start(s, t + 1)
        for t in reversed(range(stages)):
            for s in streams:
                halve, rows, _ = self.plans[s][t]
                if not halve:
                    continue
                _, device = self.partner(*self.orders[s][t])
                here = pl.ds(self.off[s], rows)
                copy = pltpu.make_async_remote_copy(
                    src_ref=self.sums[s].at[here],
                    dst_ref=self.sums[s].at[here],
                    send_sem=self.sems[2].at[s, t],
                    recv_sem=self.sems[3].at[s, t],
                    device_id=device,
                    device_id_type=MESH,
                )
                copy.start()
                self.copies[s] = copy
            for s in streams:
                if self.plans[s][t][0]:
                    self.copies[s].wait()
                    self.off[s] = self.parent[s][t]


def predict_kernel(npw, orders, m_plans, g_plans, h_ref, p_ref, g_ref, *scratch):
    m_acc, scratch = scratch[:STREAMS], scratch[STREAMS:]
    m_recv, scratch = scratch[:STREAMS], scratch[STREAMS:]
    m_sum, scratch = scratch[:STREAMS], scratch[STREAMS:]
    g_acc, scratch = scratch[:STREAMS], scratch[STREAMS:]
    g_recv, scratch = scratch[:STREAMS], scratch[STREAMS:]
    g_sum, sems = scratch[:STREAMS], scratch[STREAMS:]
    nb = h_ref.shape[1] // B
    m_red = Reducer(m_acc, m_recv, m_sum, *sems[:4], orders, m_plans)
    g_red = Reducer(g_acc, g_recv, g_sum, *sems[4:], orders, g_plans)

    barrier = pltpu.get_barrier_semaphore()
    for axis, bit in orders[0]:
        pl.semaphore_signal(barrier, inc=1, device_id=m_red.partner(axis, bit)[1], device_id_type=MESH)

    hist = [split(h_ref[j]) for j in range(3)]
    place, counts = layout(projection_blocks(nb))
    left = list(counts)
    waited = False
    for j in range(3):
        for i in range(nb):
            width = (i + 1) * B if j == 0 else nb * B
            mine = tuple(x[i * B : (i + 1) * B] for x in hist[0])
            other = tuple(x[:width] for x in hist[j])
            product = dot3(mine, other, NT)
            for k in range(width // B):
                stream, row = place[(j, i, k)]
                m_acc[stream][row : row + B, :] = product[:, k * B : (k + 1) * B]
                left[stream] -= 1
                if left[stream] == 0:
                    if not waited:
                        pl.semaphore_wait(barrier, len(orders[0]))
                        waited = True
                    m_red.start(stream, 0)
    m_red.run()

    def block(j, i, k):
        if j == 0 and k > i:
            return jnp.transpose(block(0, k, i))
        stream, row = place[(j, i, k)]
        return m_sum[stream][row : row + B, :]

    scaled = split(jnp.concatenate([h_ref[j] * (WEIGHTS[j] / npw) for j in range(3)], axis=0))
    g_place, g_counts = layout(gram_blocks(nb))
    left = list(g_counts)
    highs, lows = [], []
    for i in range(nb):
        line = jnp.concatenate([block(j, i, k) for j in range(3) for k in range(nb)], axis=1)
        predicted = dot3(split(line), scaled, NN)
        p_ref[i * B : (i + 1) * B, :] = predicted
        high, low = split(predicted)
        highs.append(high)
        lows.append(low)
        others = (jnp.concatenate(highs, axis=0), jnp.concatenate(lows, axis=0))
        product = dot3((high, low), others, NT)
        for k in range(i + 1):
            stream, row = g_place[(i, k)]
            g_acc[stream][row : row + B, :] = product[:, k * B : (k + 1) * B]
            left[stream] -= 1
            if left[stream] == 0:
                g_red.start(stream, 0)
    g_red.run()
    row = 0
    for stream in range(STREAMS):
        rows = g_counts[stream] * B
        g_ref[row : row + rows, :] = g_sum[stream][...] * (1.0 / npw)
        row += rows


def inverse_factor(tile, work):
    rows_of = lax.broadcasted_iota(jnp.int32, (B, B), 0)
    cols_of = lax.broadcasted_iota(jnp.int32, (B, B), 1)
    work[:, :B] = tile
    work[:, B:] = jnp.where(rows_of == cols_of, 1.0, 0.0)
    sub = lax.broadcasted_iota(jnp.int32, (8, B), 0)
    inverse = []
    for k in range(0, B, 8):
        left, right = work[k : k + 8, :B], work[k : k + 8, B:]
        cols = [jnp.broadcast_to(left[:, k + r : k + r + 1], (8, B)) for r in range(8)]
        pivots = None
        for r in range(8):
            def line(x):
                return jnp.broadcast_to(x[r : r + 1, :], (8, B))

            pivot = line(cols[r])
            pivots = pivot if r == 0 else jnp.where(sub == r, pivot, pivots)
            if r < 7:
                scale = jnp.where(sub > r, cols[r] / pivot, 0.0)
                for s in range(r + 1, 8):
                    cols[s] = cols[s] - scale * line(cols[s])
                left = left - scale * line(left)
                right = right - scale * line(right)
        root = 1.0 / jnp.sqrt(pivots)
        left, right = left * root, right * root
        inverse.append(right)
        if k + 8 < B:
            lh = left.astype(jnp.bfloat16).astype(jnp.float32)
            rh = right.astype(jnp.bfloat16).astype(jnp.float32)
            ll, rl = left - lh, right - rh
            zero = jnp.zeros_like(lh)
            tall = jnp.transpose(jnp.concatenate([lh, ll, lh, zero], axis=0)).astype(jnp.bfloat16)
            wide = jnp.concatenate(
                [jnp.concatenate([lh, lh, ll, zero], axis=0), jnp.concatenate([rh, rh, rl, zero], axis=0)], axis=1
            ).astype(jnp.bfloat16)
            update = lax.dot_general(tall, wide, NN, preferred_element_type=jnp.float32)
            work[k + 8 :, :] = work[k + 8 :, :] - update[k + 8 :, :]
    return jnp.concatenate(inverse, axis=0)


def solve_kernel(p_ref, g_ref, out_ref, gram, rest, work):
    nb = p_ref.shape[0] // B
    place = {block: index * B for index, block in enumerate(gram_blocks(nb))}
    gram[...] = g_ref[...]
    rest[...] = p_ref[...]

    def tile(ref, row):
        return ref.at[row : row + B]

    for k in range(nb):
        inverse = split(inverse_factor(tile(gram, place[(k, k)])[...], work))
        solved = dot3(inverse, split(tile(rest, k * B)[...]), NN)
        tile(out_ref, k * B)[...] = solved
        solved = split(solved)
        panel = {i: split(dot3(split(tile(gram, place[(i, k)])[...]), inverse, NT)) for i in range(k + 1, nb)}
        for i in range(k + 1, nb):
            here = tile(rest, i * B)
            here[...] = here[...] - dot3(panel[i], solved, NN)
            for j in range(k + 1, i + 1):
                here = tile(gram, place[(i, j)])
                here[...] = here[...] - dot3(panel[i], panel[j], NT)


def on_device(history):
    n_row, n_col = lax.axis_size("row"), lax.axis_size("col")
    norb, width = history.shape[1:]
    npw = width * n_row * n_col
    nb = norb // B
    orders = exchange_orders(n_row, n_col)
    stages = len(orders[0])
    m_counts = layout(projection_blocks(nb))[1]
    g_counts = layout(gram_blocks(nb))[1]
    m_plans = [plan(count * B, stages, 4) for count in m_counts]
    g_plans = [plan(count * B, stages, 2) for count in g_counts]
    f32 = jnp.float32
    vmem = pl.BlockSpec(memory_space=pltpu.VMEM)
    scratch = (
        [pltpu.VMEM((count * B, B), f32) for count in m_counts]
        + [pltpu.VMEM((rows, B), f32) for _, rows in m_plans]
        + [pltpu.VMEM((count * B, B), f32) for count in m_counts]
        + [pltpu.VMEM((count * B, B), f32) for count in g_counts]
        + [pltpu.VMEM((rows, B), f32) for _, rows in g_plans]
        + [pltpu.VMEM((count * B, B), f32) for count in g_counts]
        + [pltpu.SemaphoreType.DMA((STREAMS, stages))] * 8
    )
    predicted, gram = pl.pallas_call(
        functools.partial(predict_kernel, npw, orders, [p[0] for p in m_plans], [p[0] for p in g_plans]),
        out_shape=(
            jax.ShapeDtypeStruct((norb, width), f32),
            jax.ShapeDtypeStruct((sum(g_counts) * B, B), f32),
        ),
        in_specs=[vmem],
        out_specs=(vmem, vmem),
        scratch_shapes=scratch,
        compiler_params=pltpu.CompilerParams(collective_id=0, has_side_effects=True, vmem_limit_bytes=48 << 20),
    )(history)
    return pl.pallas_call(
        solve_kernel,
        out_shape=jax.ShapeDtypeStruct((norb, width), f32),
        in_specs=[vmem, vmem],
        out_specs=vmem,
        scratch_shapes=[
            pltpu.VMEM((sum(g_counts) * B, B), f32),
            pltpu.VMEM((norb, width), f32),
            pltpu.VMEM((B, 2 * B), f32),
        ],
        compiler_params=pltpu.CompilerParams(vmem_limit_bytes=32 << 20),
    )(predicted, gram)


def solution(mesh):
    return jax.shard_map(
        on_device,
        mesh=mesh,
        in_specs=(P(None, None, ("row", "col")),),
        out_specs=P(None, ("row", "col")),
        check_vma=False,
    )
```

```python
import functools

import jax
import jax.numpy as jnp
import numpy as np
from jax import lax
from jax.experimental import pallas as pl
from jax.experimental.pallas import tpu as pltpu
from jax.sharding import PartitionSpec as P

MESH = pl.DeviceIdType.MESH
B = 128
M_STREAMS, M_HALVINGS = 9, 4
G_STREAMS, G_HALVINGS = 6, 2
WEIGHTS = (2.5, -2.0, 0.5)
NT = (((1,), (1,)), ((), ()))
NN = (((1,), (0,)), ((), ()))


def split(x):
    high = x.astype(jnp.bfloat16)
    return high, (x - high.astype(jnp.float32)).astype(jnp.bfloat16)


def dot3(a, b, dims):
    mul = functools.partial(lax.dot_general, dimension_numbers=dims, preferred_element_type=jnp.float32)
    return mul(a[0], b[0]) + (mul(a[0], b[1]) + mul(a[1], b[0]))


def exchange_orders(n_row, n_col, streams):
    row = [("row", bit) for bit in range(1, n_row.bit_length() - 1)]
    col = [("col", bit) for bit in range(n_col.bit_length() - 1)]
    half = (len(row) + 1) // 2
    inner, outer = row[:half], row[half:]
    first = [("row", 0)]
    ways = [
        inner + outer + col,
        outer + col[:1] + inner + col[1:],
        col[:1] + inner + outer + col[1:],
    ]
    return [first + ways[s % 3] for s in range(streams)]


def plan(rows, stages, halvings):
    steps, offset = [], 0
    for stage in range(stages):
        halve = stage < halvings and rows % 16 == 0 and rows >= 16
        if halve:
            rows //= 2
        steps.append((halve, rows, offset))
        offset += rows
    return steps, offset


def layout(blocks, streams):
    place, counts = {}, []
    for stream, part in enumerate(np.array_split(np.arange(len(blocks)), streams)):
        counts.append(len(part))
        for slot, index in enumerate(part):
            place[blocks[index]] = (stream, slot * B)
    return place, counts


def projection_blocks(nb):
    return [(0, i, k) for i in range(nb) for k in range(i + 1)] + [
        (j, i, k) for j in (1, 2) for i in range(nb) for k in range(nb)
    ]


def gram_blocks(nb):
    return [(i, k) for i in range(nb) for k in range(i + 1)]


class Reducer:
    def __init__(self, accs, recvs, sums, send_sem, recv_sem, gsend_sem, grecv_sem, orders, plans):
        self.accs, self.recvs, self.sums, self.orders, self.plans = accs, recvs, sums, orders, plans
        self.sems = (send_sem, recv_sem, gsend_sem, grecv_sem)
        self.off = [0] * len(accs)
        self.parent = [[] for _ in accs]
        self.copies = {}
        self.index = {axis: lax.axis_index(axis) for axis in ("row", "col")}

    def partner(self, axis, bit):
        me = self.index[axis]
        side = lax.rem(lax.div(me, 1 << bit), 2)
        other = me + (1 - 2 * side) * (1 << bit)
        device = (other, self.index["col"]) if axis == "row" else (self.index["row"], other)
        return side, device

    def start(self, s, t):
        side, device = self.partner(*self.orders[s][t])
        halve, rows, at = self.plans[s][t]
        off = self.off[s]
        self.parent[s].append(off)
        sent = off
        if halve:
            sent = pl.multiple_of(off + (1 - side) * rows, 8)
            self.off[s] = pl.multiple_of(off + side * rows, 8)
        copy = pltpu.make_async_remote_copy(
            src_ref=self.accs[s].at[pl.ds(sent, rows)],
            dst_ref=self.recvs[s].at[pl.ds(at, rows)],
            send_sem=self.sems[0].at[s, t],
            recv_sem=self.sems[1].at[s, t],
            device_id=device,
            device_id_type=MESH,
        )
        copy.start()
        self.copies[s] = copy

    def finish(self, s, t):
        self.copies[s].wait()
        _, rows, at = self.plans[s][t]
        here = pl.ds(self.off[s], rows)
        target = self.sums[s] if t + 1 == len(self.orders[s]) else self.accs[s]
        target[here] = self.accs[s][here] + self.recvs[s][pl.ds(at, rows)]

    def run(self):
        stages = len(self.orders[0])
        streams = range(len(self.accs))
        for t in range(stages):
            for s in streams:
                self.finish(s, t)
                if t + 1 < stages:
                    self.start(s, t + 1)
        for t in reversed(range(stages)):
            for s in streams:
                halve, rows, _ = self.plans[s][t]
                if not halve:
                    continue
                self.gathered(s, t + 1)
                _, device = self.partner(*self.orders[s][t])
                here = pl.ds(self.off[s], rows)
                copy = pltpu.make_async_remote_copy(
                    src_ref=self.sums[s].at[here],
                    dst_ref=self.sums[s].at[here],
                    send_sem=self.sems[2].at[s, t],
                    recv_sem=self.sems[3].at[s, t],
                    device_id=device,
                    device_id_type=MESH,
                )
                copy.start()
                self.copies[s] = copy
        for s in streams:
            self.gathered(s, 0)

    def gathered(self, s, t):
        if t < len(self.plans[s]) and self.plans[s][t][0]:
            self.copies[s].wait()
            self.off[s] = self.parent[s][t]


def predict_kernel(npw, m_orders, g_orders, m_plans, g_plans, h_ref, p_ref, g_ref, *scratch):
    scratch = list(scratch)

    def take(count):
        return [scratch.pop(0) for _ in range(count)]

    m_acc, m_recv, m_sum = (take(M_STREAMS) for _ in range(3))
    g_acc, g_recv, g_sum = (take(G_STREAMS) for _ in range(3))
    sems = scratch
    nb = h_ref.shape[1] // B
    m_red = Reducer(m_acc, m_recv, m_sum, *sems[:4], m_orders, m_plans)
    g_red = Reducer(g_acc, g_recv, g_sum, *sems[4:], g_orders, g_plans)

    barrier = pltpu.get_barrier_semaphore()
    for axis, bit in m_orders[0]:
        pl.semaphore_signal(barrier, inc=1, device_id=m_red.partner(axis, bit)[1], device_id_type=MESH)

    hist = [split(h_ref[j]) for j in range(3)]
    place, counts = layout(projection_blocks(nb), M_STREAMS)
    left = list(counts)
    waited = False
    for j in range(3):
        for i in range(nb):
            width = (i + 1) * B if j == 0 else nb * B
            mine = tuple(x[i * B : (i + 1) * B] for x in hist[0])
            other = tuple(x[:width] for x in hist[j])
            product = dot3(mine, other, NT)
            for k in range(width // B):
                stream, row = place[(j, i, k)]
                m_acc[stream][row : row + B, :] = product[:, k * B : (k + 1) * B]
                left[stream] -= 1
                if left[stream] == 0:
                    if not waited:
                        pl.semaphore_wait(barrier, len(m_orders[0]))
                        waited = True
                    m_red.start(stream, 0)
    m_red.run()

    def block(j, i, k):
        if j == 0 and k > i:
            return jnp.transpose(block(0, k, i))
        stream, row = place[(j, i, k)]
        return m_sum[stream][row : row + B, :]

    scaled = split(jnp.concatenate([h_ref[j] * (WEIGHTS[j] / npw) for j in range(3)], axis=0))
    g_place, g_counts = layout(gram_blocks(nb), G_STREAMS)
    left = list(g_counts)
    highs, lows = [], []
    for i in range(nb):
        line = jnp.concatenate([block(j, i, k) for j in range(3) for k in range(nb)], axis=1)
        predicted = dot3(split(line), scaled, NN)
        p_ref[i * B : (i + 1) * B, :] = predicted
        high, low = split(predicted)
        highs.append(high)
        lows.append(low)
        others = (jnp.concatenate(highs, axis=0), jnp.concatenate(lows, axis=0))
        product = dot3((high, low), others, NT)
        for k in range(i + 1):
            stream, row = g_place[(i, k)]
            g_acc[stream][row : row + B, :] = product[:, k * B : (k + 1) * B]
            left[stream] -= 1
            if left[stream] == 0:
                g_red.start(stream, 0)
    g_red.run()
    row = 0
    for stream in range(G_STREAMS):
        rows = g_counts[stream] * B
        g_ref[row : row + rows, :] = g_sum[stream][...] * (1.0 / npw)
        row += rows


def inverse_factor(tile, work):
    rows_of = lax.broadcasted_iota(jnp.int32, (B, B), 0)
    cols_of = lax.broadcasted_iota(jnp.int32, (B, B), 1)
    work[:, :B] = tile
    work[:, B:] = jnp.where(rows_of == cols_of, 1.0, 0.0)
    sub = lax.broadcasted_iota(jnp.int32, (8, B), 0)
    inverse = []

    def line(x, r):
        return jnp.broadcast_to(x[r : r + 1, :], (8, B))

    for k in range(0, B, 16):
        top = [jnp.broadcast_to(work[k : k + 8, k + r : k + r + 1], (8, B)) for r in range(16)]
        low = [jnp.broadcast_to(work[k + 8 : k + 16, k + r : k + r + 1], (8, B)) for r in range(16)]
        top += [work[k : k + 8, :B], work[k : k + 8, B:]]
        low += [work[k + 8 : k + 16, :B], work[k + 8 : k + 16, B:]]
        pivots = [None, None]
        for r in range(16):
            upper, q = r < 8, r % 8
            pivot = line((top if upper else low)[r], q)
            pivots[r // 8] = pivot if q == 0 else jnp.where(sub == q, pivot, pivots[r // 8])
            if r == 15:
                break
            inv = 1.0 / pivot
            if upper:
                top_scale = jnp.where(sub > q, top[r] * inv, 0.0)
                low_scale = low[r] * inv
                for s in range(r + 1, 18):
                    row = line(top[s], q)
                    top[s] = top[s] - top_scale * row
                    low[s] = low[s] - low_scale * row
            else:
                low_scale = jnp.where(sub > q, low[r] * inv, 0.0)
                for s in range(r + 1, 18):
                    low[s] = low[s] - low_scale * line(low[s], q)
        root = [1.0 / jnp.sqrt(p) for p in pivots]
        left = jnp.concatenate([top[16] * root[0], low[16] * root[1]], axis=0)
        right = jnp.concatenate([top[17] * root[0], low[17] * root[1]], axis=0)
        inverse.append(right)
        if k + 16 < B:
            lh = left.astype(jnp.bfloat16).astype(jnp.float32)
            rh = right.astype(jnp.bfloat16).astype(jnp.float32)
            ll, rl = left - lh, right - rh
            tall = jnp.transpose(jnp.concatenate([lh, ll, lh], axis=0)).astype(jnp.bfloat16)
            wide = jnp.concatenate(
                [jnp.concatenate([lh, lh, ll], axis=0), jnp.concatenate([rh, rh, rl], axis=0)], axis=1
            ).astype(jnp.bfloat16)
            update = lax.dot_general(tall, wide, NN, preferred_element_type=jnp.float32)
            work[k + 16 :, :] = work[k + 16 :, :] - update[k + 16 :, :]
    return jnp.concatenate(inverse, axis=0)


def solve_kernel(p_ref, g_ref, out_ref, gram, rest, work):
    nb = p_ref.shape[0] // B
    place = {block: index * B for index, block in enumerate(gram_blocks(nb))}
    gram[...] = g_ref[...]
    rest[...] = p_ref[...]

    def tile(ref, row):
        return ref.at[row : row + B]

    for k in range(nb):
        inverse = split(inverse_factor(tile(gram, place[(k, k)])[...], work))
        solved = dot3(inverse, split(tile(rest, k * B)[...]), NN)
        tile(out_ref, k * B)[...] = solved
        solved = split(solved)
        panel = {i: split(dot3(split(tile(gram, place[(i, k)])[...]), inverse, NT)) for i in range(k + 1, nb)}
        for i in range(k + 1, nb):
            here = tile(rest, i * B)
            here[...] = here[...] - dot3(panel[i], solved, NN)
            for j in range(k + 1, i + 1):
                here = tile(gram, place[(i, j)])
                here[...] = here[...] - dot3(panel[i], panel[j], NT)


def on_device(history):
    n_row, n_col = lax.axis_size("row"), lax.axis_size("col")
    norb, width = history.shape[1:]
    npw = width * n_row * n_col
    nb = norb // B
    m_orders = exchange_orders(n_row, n_col, M_STREAMS)
    g_orders = exchange_orders(n_row, n_col, G_STREAMS)
    stages = len(m_orders[0])
    m_counts = layout(projection_blocks(nb), M_STREAMS)[1]
    g_counts = layout(gram_blocks(nb), G_STREAMS)[1]
    m_plans = [plan(count * B, stages, M_HALVINGS) for count in m_counts]
    g_plans = [plan(count * B, stages, G_HALVINGS) for count in g_counts]
    f32 = jnp.float32
    vmem = pl.BlockSpec(memory_space=pltpu.VMEM)
    scratch = (
        [pltpu.VMEM((count * B, B), f32) for count in m_counts]
        + [pltpu.VMEM((rows, B), f32) for _, rows in m_plans]
        + [pltpu.VMEM((count * B, B), f32) for count in m_counts]
        + [pltpu.VMEM((count * B, B), f32) for count in g_counts]
        + [pltpu.VMEM((rows, B), f32) for _, rows in g_plans]
        + [pltpu.VMEM((count * B, B), f32) for count in g_counts]
        + [pltpu.SemaphoreType.DMA((M_STREAMS, stages))] * 4
        + [pltpu.SemaphoreType.DMA((G_STREAMS, stages))] * 4
    )
    predicted, gram = pl.pallas_call(
        functools.partial(predict_kernel, npw, m_orders, g_orders, [p[0] for p in m_plans], [p[0] for p in g_plans]),
        out_shape=(
            jax.ShapeDtypeStruct((norb, width), f32),
            jax.ShapeDtypeStruct((sum(g_counts) * B, B), f32),
        ),
        in_specs=[vmem],
        out_specs=(vmem, vmem),
        scratch_shapes=scratch,
        compiler_params=pltpu.CompilerParams(collective_id=0, has_side_effects=True, vmem_limit_bytes=48 << 20),
    )(history)
    return pl.pallas_call(
        solve_kernel,
        out_shape=jax.ShapeDtypeStruct((norb, width), f32),
        in_specs=[vmem, vmem],
        out_specs=vmem,
        scratch_shapes=[
            pltpu.VMEM((sum(g_counts) * B, B), f32),
            pltpu.VMEM((norb, width), f32),
            pltpu.VMEM((B, 2 * B), f32),
        ],
        compiler_params=pltpu.CompilerParams(vmem_limit_bytes=32 << 20),
    )(predicted, gram)


def solution(mesh):
    return jax.shard_map(
        on_device,
        mesh=mesh,
        in_specs=(P(None, None, ("row", "col")),),
        out_specs=P(None, ("row", "col")),
        check_vma=False,
    )
```
